32 devices in a mesh: dom: 32 (over z, y, x, core).
Axes of the slice: x: 2, y: 2, z: 4, core: 2. Of those that a mesh axis runs over, the one named last changes fastest.
Arguments:
- start_point: float32 [16384, 128], P('dom'), may hold values from -6 to 6
- residual: float32 [16384, 128], P('dom'), may hold values from -40 to 40
- direction: float32 [16384, 128], P('dom'), may hold values from -40 to 40
- send_list: int32 [32, 4, 3], P('dom'), may hold values from 0 to 3, as said below
- block_cols: int32 [128, 6], P('dom'), may hold values from 0 to 15, as said below
- block_vals: float32 [128, 6, 128, 128], P('dom'), may hold values from -0.2 to 8.1, as said below
Outputs:
- new_point: float32 [16384, 128], P('dom')
- new_residual: float32 [16384, 128], P('dom')
- new_direction: float32 [16384, 128], P('dom')
The draws below stay inside these ranges and needn't reach their ends.
Inputs may be any that keep to these rules, and one draw needn't show every extreme that they name: send_list[t, m] lists, in its first entries, the distinct blocks of partition t that the partition at offset -off (off as in the first step) reads; between 1 and 3 of them are read for each pair, and some pair reads 3; the other entries are valid block numbers that are never read. `block_cols`: entry 0 of a block row names the row's own block; a block that couples two partitions appears in both partitions' rows, transposed; the assembled matrix is symmetric positive definite. `block_vals`: stored blocks that no coupling uses are zero.
All inputs are finite; a program needn't handle non-finite values.
Results may differ from the reference program's by a relative error of at most 0.0003.
Values sent between devices are 32-bit elements; how exact they have to be, the bound alone decides.
No kernel may reach another device: no remote copies, remote signals or barrier semaphores. Data moves between devices by JAX's collectives and lax.ppermute only.
A program may use at most 128 MiB of HBM per device.

```python
import math
import jax
import jax.numpy as jnp
from jax import lax

BLOCK = 128
NB = 4
NRHS = 128
HOPS = 2
CAP = 3
STEPS = 6
SLOTS = 6
BASIS = 13
NBLK = 128


def ordering(key, dev_count):
    scores = jax.random.randint(key, (dev_count, NB), 0, 1 << 20) * NB + jnp.arange(NB)[None, :]
    order_ids = jnp.argsort(scores, axis=1).astype(jnp.int32)
    rank_ids = jnp.argsort(order_ids, axis=1).astype(jnp.int32)
    return (order_ids, rank_ids)


def structure(key):
    dev_count = NBLK // NB
    base_key = jax.random.fold_in(key, 4242)
    devices = jnp.arange(dev_count, dtype=jnp.int32)
    hop_data = []
    for hop_index in range(HOPS):
        count_key, chosen_key, left_key, right_key = jax.random.split(jax.random.fold_in(base_key, hop_index), 4)
        counts = jax.random.randint(count_key, (dev_count,), 1, CAP + 1)
        chosen = jax.random.randint(chosen_key, (), 0, dev_count)
        counts = jnp.where(devices == chosen, CAP, counts).astype(jnp.int32)
        left_order, left_rank = ordering(left_key, dev_count)
        right_order, right_rank = ordering(right_key, dev_count)
        hop_data.append((counts, left_order, left_rank, right_order, right_rank))
    local_order, local_rank = ordering(jax.random.fold_in(base_key, 99), dev_count)
    return (hop_data, local_order, local_rank)


def draw_send_list(key, part):
    dev_count = NBLK // NB
    devices = jnp.arange(dev_count, dtype=jnp.int32)
    hop_data, local_order, local_rank = structure(key)
    right_parts = []
    left_parts = []
    for hop_index in range(HOPS):
        counts, left_order, left_rank, right_order, right_rank = hop_data[hop_index]
        distance = hop_index + 1
        right_parts.append(right_order[(devices - distance) % dev_count, :CAP])
        left_parts.append(left_order[:, :CAP])
    return jnp.stack(right_parts + left_parts, axis=1).astype(jnp.int32)


def draw_block_cols(key, part):
    dev_count = NBLK // NB
    devices = jnp.arange(dev_count, dtype=jnp.int32)
    hop_data, local_order, local_rank = structure(key)
    own_blocks = jnp.broadcast_to(jnp.arange(NB, dtype=jnp.int32)[None, :], (dev_count, NB))
    local_partner = jnp.take_along_axis(local_order, jnp.bitwise_xor(local_rank, 1), axis=1)
    plus_cols = []
    minus_cols = []
    for hop_index in range(HOPS):
        counts, left_order, left_rank, right_order, right_rank = hop_data[hop_index]
        distance = hop_index + 1
        is_valid = left_rank < counts[:, None]
        plus_cols.append(jnp.where(is_valid, NB + hop_index * CAP + left_rank, own_blocks))
        left_dev = (devices - distance) % dev_count
        edge_rank = right_rank[left_dev]
        valid_right = edge_rank < counts[left_dev][:, None]
        minus_cols.append(jnp.where(valid_right, NB + (HOPS + hop_index) * CAP + edge_rank, own_blocks))
    joined = jnp.stack([own_blocks, local_partner] + plus_cols + minus_cols, axis=2)
    return joined.reshape(NBLK, SLOTS).astype(jnp.int32)


def draw_block_vals(key, part):
    dev_count = NBLK // NB
    devices = jnp.arange(dev_count, dtype=jnp.int32)
    hop_data, local_order, local_rank = structure(key)
    value_key = jax.random.fold_in(key, 5151)
    diag_key, noise_key, local_key = jax.random.split(value_key, 3)
    diag_vals = jnp.exp(jax.random.uniform(diag_key, (dev_count, NB, BLOCK), minval=math.log(1.6), maxval=math.log(8.0)))
    noise = jax.random.truncated_normal(noise_key, -6.0, 6.0, (dev_count, NB, BLOCK, BLOCK)) * (0.02 / math.sqrt(BLOCK))
    eye_block = jnp.eye(BLOCK, dtype=jnp.float32)
    diag_blocks = eye_block[None, None] * diag_vals[..., None] + 0.5 * (noise + jnp.swapaxes(noise, -1, -2))
    local_table = jax.random.truncated_normal(local_key, -6.0, 6.0, (dev_count, NB // 2, BLOCK, BLOCK)) * (0.15 / math.sqrt(BLOCK))
    pair_ids = local_rank // 2
    is_first = local_rank % 2 == 0
    picked = local_table[devices[:, None], pair_ids]
    local_vals = jnp.where(is_first[..., None, None], picked, jnp.swapaxes(picked, -1, -2))
    plus_vals = []
    minus_vals = []
    for hop_index in range(HOPS):
        counts, left_order, left_rank, right_order, right_rank = hop_data[hop_index]
        distance = hop_index + 1
        coupling = jax.random.truncated_normal(jax.random.fold_in(value_key, 100 + hop_index), -6.0, 6.0, (dev_count, CAP, BLOCK, BLOCK)) * (0.15 / math.sqrt(BLOCK))
        is_valid = (left_rank < counts[:, None]).astype(jnp.float32)
        edge_left = jnp.minimum(left_rank, CAP - 1)
        plus_vals.append(coupling[devices[:, None], edge_left] * is_valid[..., None, None])
        left_dev = (devices - distance) % dev_count
        edge_rank = right_rank[left_dev]
        valid_right = (edge_rank < counts[left_dev][:, None]).astype(jnp.float32)
        edge_right = jnp.minimum(edge_rank, CAP - 1)
        minus_vals.append(jnp.swapaxes(coupling[left_dev[:, None], edge_right], -1, -2) * valid_right[..., None, None])
    joined = jnp.stack([diag_blocks, local_vals] + plus_vals + minus_vals, axis=2)
    return joined.reshape(NBLK, SLOTS, BLOCK, BLOCK).astype(jnp.float32)


def rising_field(key, marker):
    row_count = NBLK * BLOCK
    dev_count = NBLK // NB
    sub_key = jax.random.fold_in(key, marker)
    owner_ids = jnp.arange(row_count) // (NB * BLOCK)
    ramp_vals = 1.0 + 2.0 * owner_ids.astype(jnp.float32) / max(dev_count - 1, 1)
    values = jax.random.truncated_normal(sub_key, -6.0, 6.0, (row_count, NRHS))
    return (values * ramp_vals[:, None]).astype(jnp.float32)


def draw_residual(key, part):
    return rising_field(key, 311)


def draw_direction(key, part):
    return rising_field(key, 733)


def steps_of(rng, dims, pieces, smallest, top_value):
    factor_of, own = 1.0, jax.random.fold_in(rng, 6)
    for position, parts in pieces:
        steps = jnp.exp(jax.random.uniform(jax.random.fold_in(own, position), (parts,), jnp.float32, smallest / len(pieces), top_value / len(pieces)))
        factor_of = factor_of * jnp.repeat(steps, dims[position] // parts).reshape([-1 if axis == position else 1 for axis in range(len(dims))])
    return factor_of


def scatter_about(own_key, dims, deviation, bound, cuts=(), kind=jnp.bfloat16):
    array = deviation * jax.random.normal(own_key, dims, jnp.float32)
    if cuts:
        array = array * steps_of(own_key, dims, cuts, -0.22, 0.18)
    return jnp.clip(array, -bound, bound).astype(kind)


def setup_inputs(seed: int = 0) -> dict:
    key_of = jax.random.split(jax.random.key(seed), 7)
    return {
        "start_point": scatter_about(key_of[0], (NBLK * BLOCK, NRHS), 1.0, 6.0, ((0, 32),), jnp.float32),
        "residual": draw_residual(jax.random.fold_in(key_of[6], 71), 0),
        "direction": draw_direction(jax.random.fold_in(key_of[6], 71), 0),
        "send_list": draw_send_list(jax.random.fold_in(key_of[6], 71), 0),
        "block_cols": draw_block_cols(jax.random.fold_in(key_of[6], 71), 0),
        "block_vals": draw_block_vals(jax.random.fold_in(key_of[6], 71), 0),
    }


center_value = 4.5
half_range = 4.5


def slot_offset(slot_index):
    return slot_index + 1 if slot_index < HOPS else HOPS - 1 - slot_index


def global_columns(block_cols, send_list):
    dev_count = NBLK // NB
    devices = jnp.arange(dev_count, dtype=jnp.int32)
    tables = [devices[:, None] * NB + jnp.arange(NB, dtype=jnp.int32)[None, :]]
    for slot_index in range(2 * HOPS):
        partner = (devices + slot_offset(slot_index)) % dev_count
        tables.append(partner[:, None] * NB + send_list[partner, slot_index, :].astype(jnp.int32))
    joined = jnp.concatenate(tables, axis=1).astype(jnp.int32)
    owners = jnp.arange(NBLK, dtype=jnp.int32) // NB
    return jnp.take_along_axis(joined[owners], block_cols.astype(jnp.int32), axis=1)


def apply_matrix(vector, columns, block_vals):
    blocked = vector.reshape(NBLK, BLOCK, vector.shape[1])
    running = jnp.zeros(blocked.shape, jnp.float32)
    for slot_index in range(SLOTS):
        picked = jnp.take(blocked, columns[:, slot_index], axis=0)
        running = running + jnp.einsum("ibc,icw->ibw", block_vals[:, slot_index], picked, precision=lax.Precision.HIGHEST)
    return running.reshape(vector.shape)


def next_vector(vector, columns, block_vals):
    return (apply_matrix(vector, columns, block_vals) - center_value * vector) / half_range


def basis_change():
    positions = jnp.arange(BASIS)
    row_ids = positions[:, None]
    col_ids = positions[None, :]
    active = (col_ids < STEPS) | ((col_ids > STEPS) & (col_ids < BASIS - 1))
    change_table = jnp.where(active & (row_ids == col_ids), center_value, 0.0)
    change_table = change_table + jnp.where(active & (row_ids == col_ids + 1), half_range, 0.0)
    return change_table.astype(jnp.float32)


def coefficient_steps(gram_matrix):
    change_table = basis_change()
    column_count = gram_matrix.shape[0]
    positions = jnp.arange(BASIS)
    point_c = jnp.zeros((column_count, BASIS), jnp.float32)
    resid_c = jnp.broadcast_to((positions == STEPS + 1).astype(jnp.float32), (column_count, BASIS))
    direc_c = jnp.broadcast_to((positions == 0).astype(jnp.float32), (column_count, BASIS))
    highest = lax.Precision.HIGHEST
    for step_index in range(STEPS):
        current = jnp.sum(resid_c * jnp.einsum("nab,nb->na", gram_matrix, resid_c, precision=highest), axis=1)
        moved_dir = jnp.einsum("ab,nb->na", change_table, direc_c, precision=highest)
        curvature = jnp.sum(direc_c * jnp.einsum("nab,nb->na", gram_matrix, moved_dir, precision=highest), axis=1)
        alpha_step = current / curvature
        point_c = point_c + alpha_step[:, None] * direc_c
        resid_c = resid_c - alpha_step[:, None] * moved_dir
        following = jnp.sum(resid_c * jnp.einsum("nab,nb->na", gram_matrix, resid_c, precision=highest), axis=1)
        direc_c = resid_c + (following / current)[:, None] * direc_c
    return point_c, resid_c, direc_c


def combine_basis(weights, basis_all):
    running = jnp.zeros(basis_all[0].shape, jnp.float32)
    for basis_index in range(BASIS):
        running = running + weights[:, basis_index][None, :] * basis_all[basis_index]
    return running


def reference(start_point, residual, direction, send_list, block_cols, block_vals):
    columns = global_columns(block_cols, send_list)
    p_basis = [direction]
    for power_step in range(STEPS):
        p_basis.append(next_vector(p_basis[-1], columns, block_vals))
    r_basis = [residual]
    for power_step in range(STEPS - 1):
        r_basis.append(next_vector(r_basis[-1], columns, block_vals))
    basis_all = p_basis + r_basis
    gram_matrix = jnp.stack([jnp.stack([jnp.sum(basis_all[first] * basis_all[second], axis=0) for second in range(BASIS)], axis=1) for first in range(BASIS)], axis=1)
    point_c, resid_c, direc_c = coefficient_steps(gram_matrix)
    new_point = start_point + combine_basis(point_c, basis_all)
    new_residual = combine_basis(resid_c, basis_all)
    new_direction = combine_basis(direc_c, basis_all)
    return new_point, new_residual, new_direction
```

```python
import functools
import jax
import jax.numpy as jnp
from jax import lax
from jax.experimental import pallas as pl
from jax.experimental.pallas import tpu as pltpu
from jax.sharding import PartitionSpec as P

STEPS = 6
CENTER = 4.5
HALF = 4.5
F32 = jnp.float32
BF16 = jnp.bfloat16
VM = pl.BlockSpec(memory_space=pltpu.VMEM)
SM = pl.BlockSpec(memory_space=pltpu.SMEM)


def call(body, out_shape, in_specs, out_specs, scratch=(), flops=0, bytes_=0, name=None, grid=None):
    extra = {} if grid is None else {"grid": grid}
    return pl.pallas_call(
        body,
        out_shape=out_shape,
        in_specs=in_specs,
        out_specs=out_specs,
        scratch_shapes=list(scratch),
        cost_estimate=pl.CostEstimate(flops=flops, bytes_accessed=bytes_, transcendentals=0),
        name=name,
        **extra,
    )


def pack_kernel(core, p_ref, r_ref, mine_ref, send_ref):
    half = p_ref.shape[1] // 2
    p, r = p_ref[...], r_ref[...]
    low = lax.broadcasted_iota(jnp.int32, p.shape, 1) < half
    first = jnp.where(low, p, pltpu.roll(r, half, 1))
    second = jnp.where(low, pltpu.roll(p, half, 1), r)
    is_first = core[0] == 0
    mine_ref[...] = jnp.where(is_first, first, second)
    send_ref[...] = jnp.where(is_first, second, first)


def copy_halo(core, lists, own, right_ref, left_ref):
    nb = right_ref.shape[0] - lists.shape[2]
    k = core[0]
    for target, whole, part, m in ((right_ref, 1, 0, 3), (left_ref, 0, 1, 1)):
        whole_slot = jnp.bitwise_xor(k, whole)
        part_slot = jnp.bitwise_xor(k, part)
        for b in range(nb):
            target[b] = own[whole_slot * nb + b]
        for e in range(lists.shape[2]):
            target[nb + e] = own[part_slot * nb + lists[part_slot, m, e]]


def first_kernel(core, lists, mine_ref, other_ref, own_ref, right_ref, left_ref):
    nb = mine_ref.shape[0]
    own_ref[:nb] = mine_ref[...]
    own_ref[nb:] = other_ref[...]
    copy_halo(core, lists, own_ref, right_ref, left_ref)


def index_kernel(core, lists, from_right, from_left, cols, out):
    k = core[0]
    cap = lists.shape[2]
    _, nb, slots = cols.shape
    right = 2 * nb
    left = 3 * nb + cap
    for s in range(2):
        t = jnp.bitwise_xor(k, s)
        is0 = t == 0
        other = 1 - s
        for b in range(nb):
            for j in range(slots):
                c = cols[s, b, j]
                place = s * nb + c
                for m in range(4):
                    for e in range(cap):
                        if m == 0:
                            v = jnp.where(is0, other * nb + lists[other, 0, e], right + from_right[k, 0, e])
                        elif m == 1:
                            v = jnp.where(is0, right + from_right[k, 1, e], right + nb + e)
                        elif m == 2:
                            v = jnp.where(is0, left + from_left[1 - k, 2, e], other * nb + lists[other, 2, e])
                        else:
                            v = jnp.where(is0, left + nb + e, left + from_left[1 - k, 3, e])
                        place = jnp.where(c == nb + m * cap + e, v, place)
                out[s * nb + b, j] = place


def matrix_kernel(a_ref, hi_ref, lo_ref):
    slots, rows, cols = a_ref.shape[1:]
    diag = lax.broadcasted_iota(jnp.int32, (rows, cols), 0) == lax.broadcasted_iota(
        jnp.int32, (rows, cols), 1
    )
    for j in range(slots):
        a = a_ref[0, j]
        if j == 0:
            a = a - jnp.where(diag, F32(CENTER), F32(0.0))
        a = a * F32(1.0 / HALF)
        hi = a.astype(BF16)
        hi_ref[0, :, j * cols : (j + 1) * cols] = hi
        lo_ref[0, :, j * cols : (j + 1) * cols] = (a - hi.astype(F32)).astype(BF16)


def step_kernel(last, core, lists, index, own_ref, fr_ref, fl_ref, h0, l0, h1, l1, new_ref, *rest):
    if last:
        (table,) = rest
    else:
        right_ref, left_ref, table = rest
    n_own, rows, width = own_ref.shape
    place = 0
    for ref in (own_ref, fr_ref, fl_ref):
        for b in range(ref.shape[0]):
            v = ref[b]
            hi = v.astype(BF16)
            table[place, :, :width] = hi
            table[place, :, width:] = (v - hi.astype(F32)).astype(BF16)
            place += 1
    half = n_own // 2
    slots = index.shape[1]
    for i in range(n_own):
        h, l = (h0, l0) if i < half else (h1, l1)
        acc = None
        for j in range(0, slots, 2):
            cols = [table[index[i, q]] for q in range(j, min(j + 2, slots))]
            tile = jnp.concatenate(cols, axis=0) if len(cols) > 1 else cols[0]
            span = slice(j * rows, (j + len(cols)) * rows)
            for part in (h, l):
                d = jnp.dot(part[i % half, :, span], tile, preferred_element_type=F32)
                acc = d if acc is None else acc + d
        new_ref[i] = acc[:, :width] + acc[:, width:]
    if not last:
        copy_halo(core, lists, new_ref, right_ref, left_ref)


def fold(x):
    return jnp.sum(x.reshape(-1, 8, x.shape[-1]), axis=0)


def moment_kernel(first, *refs):
    if first:
        now_ref, out = refs
        prev_ref = None
    else:
        now_ref, prev_ref, out = refs
    blocks, rows, width = now_ref.shape
    half = width // 2
    acc = [jnp.zeros((8, width), F32) for _ in range(4)]
    for b in range(blocks):
        s = now_ref[b]
        turned = pltpu.roll(s, half, 1)
        acc[1] += fold(s * s)
        acc[3] += fold(s * turned)
        if prev_ref is not None:
            q = prev_ref[b]
            acc[0] += fold(s * q)
            acc[2] += fold(s * pltpu.roll(q, half, 1))
    for i in range(4):
        out[i : i + 1, :] = jnp.sum(acc[i], axis=0, keepdims=True)
    out[4:8, :] = jnp.zeros((4, width), F32)


def coefficient_kernel(m_ref, out_ref, gram_ref):
    width = m_ref.shape[1]
    half = width // 2
    count = STEPS + 1

    def row(j, i):
        return m_ref[8 * j + i : 8 * j + i + 1, :]

    def moment(n):
        j = (n + 1) // 2
        return row(j, 0 if n % 2 else 1)

    def cross(n):
        j = (n + 1) // 2
        return row(j, 2 if n % 2 else 3)

    size = gram_ref.shape[1]
    gram_ref[...] = jnp.zeros(gram_ref.shape, F32)
    for a in range(count):
        for b in range(count):
            gram_ref[a, b : b + 1, :] = moment(a + b)
            if b < STEPS:
                gram_ref[a, count + b : count + b + 1, :] = cross(a + b)
            if a < STEPS:
                gram_ref[count + a, b : b + 1, :] = cross(a + b)
            if a < STEPS and b < STEPS:
                gram_ref[count + a, count + b : count + b + 1, :] = pltpu.roll(moment(a + b), half, 1)
    ids = lax.broadcasted_iota(jnp.int32, (size, width), 0)
    active = (ids < STEPS) | ((ids > STEPS) & (ids < 2 * STEPS))

    def change(v):
        v = jnp.where(active, v, F32(0.0))
        return F32(CENTER) * v + F32(HALF) * pltpu.roll(v, 1, 0)

    def times(v):
        out = None
        for a in range(2 * STEPS + 1):
            t = gram_ref[a] * v[a : a + 1, :]
            out = t if out is None else out + t
        return out

    def dot(u, v):
        return jnp.sum(u * v, axis=0, keepdims=True)

    x = jnp.zeros((size, width), F32)
    r = jnp.where(ids == STEPS + 1, F32(1.0), F32(0.0))
    d = jnp.where(ids == 0, F32(1.0), F32(0.0))
    current = dot(r, times(r))
    for _ in range(STEPS):
        moved = change(d)
        alpha = current / dot(d, times(moved))
        x = x + alpha * d
        r = r - alpha * moved
        following = dot(r, times(r))
        d = r + (following / current) * d
        current = following
    low = lax.broadcasted_iota(jnp.int32, (8, width), 1) < half
    sub = lax.broadcasted_iota(jnp.int32, (8, width), 0)
    for q, v in enumerate((x, r, d)):
        lows = v[:8]
        lows = jnp.where(sub < count, lows, F32(0.0))
        highs = pltpu.roll(v, size - count, 0)[:8]
        highs = jnp.where(sub < STEPS, pltpu.roll(highs, half, 1), F32(0.0))
        out_ref[8 * q : 8 * q + 8, :] = jnp.where(low, lows, highs)


def combine_kernel(*refs):
    basis, (w_ref, mine_ref, send_ref) = refs[:-3], refs[-3:]
    blocks, rows, width = basis[0].shape
    half = width // 2
    nb = blocks // 2
    for b in range(blocks):
        vs = [s[b] for s in basis]
        for q in range(3):
            out = None
            for j, v in enumerate(vs):
                t = v * w_ref[8 * q + j : 8 * q + j + 1, :]
                out = t if out is None else out + t
            out = out + pltpu.roll(out, half, 1)
            if b < nb:
                mine_ref[q * nb + b] = out
            else:
                send_ref[q * nb + b - nb] = out


def shards(devices, start_point, residual, direction, send_list, block_cols, block_vals):
    nb, slots, rows, _ = block_vals.shape
    cap = send_list.shape[2]
    width = direction.shape[1]
    half = width // 2
    ghosts = nb + cap
    sds = jax.ShapeDtypeStruct
    vec = lambda n: sds((n, rows, width), F32)
    core = (lax.axis_index("dom") % 2).astype(jnp.int32).reshape(1)
    swap = [(i, i ^ 1) for i in range(devices)]
    to_right = [(i, (i + 2) % devices) for i in range(devices)]
    to_left = [(i, (i - 2) % devices) for i in range(devices)]
    permute = lambda v, pairs: lax.ppermute(v, "dom", pairs)

    mine, send = call(
        pack_kernel,
        [sds(direction.shape, F32)] * 2,
        [SM, VM, VM],
        [VM, VM],
        bytes_=4 * direction.size * 4,
        flops=direction.size,
        name="pack",
    )(core, direction, residual)
    other = permute(send, swap)
    lists = jnp.stack([send_list[0], permute(send_list[0], swap)])
    own, right, left = call(
        first_kernel,
        [vec(2 * nb), vec(ghosts), vec(ghosts)],
        [SM, SM, VM, VM],
        [VM, VM, VM],
        bytes_=6 * direction.size * 4,
        flops=direction.size,
        name="first",
    )(core, lists, mine.reshape(nb, rows, width), other.reshape(nb, rows, width))
    fr, fl = permute(left, to_left), permute(right, to_right)
    vals_other = permute(block_vals, swap)
    cols = jnp.stack([block_cols, permute(block_cols, swap)])
    lists_right, lists_left = permute(lists, to_left), permute(lists, to_right)
    index = call(
        index_kernel,
        sds((2 * nb, slots), jnp.int32),
        [SM] * 5,
        SM,
        flops=1000,
        name="index",
    )(core, lists, lists_right, lists_left, cols)

    def split(vals):
        spec = pl.BlockSpec((1, rows, slots * rows), lambda i: (i, 0, 0))
        return call(
            matrix_kernel,
            [sds((nb, rows, slots * rows), BF16)] * 2,
            [pl.BlockSpec((1, slots, rows, rows), lambda i: (i, 0, 0, 0))],
            [spec, spec],
            grid=(nb,),
            flops=4 * vals.size,
            bytes_=8 * vals.size,
            name="matrix",
        )(vals)

    parts = split(block_vals) + split(vals_other)
    basis = [own]
    moments = []

    def moment(j):
        args = basis[j : j + 1] + basis[j - 1 : j] if j else basis[:1]
        moments.append(
            call(
                functools.partial(moment_kernel, j == 0),
                sds((8, width), F32),
                [VM] * len(args),
                VM,
                flops=8 * own.size,
                bytes_=8 * own.size,
                name="moment",
            )(*args)
        )

    for j in range(STEPS):
        last = j == STEPS - 1
        out = [vec(2 * nb)] + ([] if last else [vec(ghosts), vec(ghosts)])
        res = call(
            functools.partial(step_kernel, last),
            out,
            [SM] * 3 + [VM] * 7,
            [VM] * len(out),
            scratch=[pltpu.VMEM((2 * nb + 2 * ghosts, rows, 2 * width), BF16)],
            flops=2 * 4 * 2 * nb * slots * rows * rows * width,
            bytes_=8 * 2 * nb * slots * rows * rows,
            name="step",
        )(core, lists, index, basis[-1], fr, fl, *parts)
        moment(j)
        basis.append(res[0])
        if not last:
            fr, fl = permute(res[2], to_left), permute(res[1], to_right)
    moment(STEPS)
    total = reduce_moments(jnp.concatenate(moments, axis=0), devices)
    weights = call(
        coefficient_kernel,
        sds((24, width), F32),
        [VM],
        VM,
        scratch=[pltpu.VMEM((2 * STEPS + 1, 16, width), F32)],
        flops=100000,
        name="coefficients",
    )(total)
    mine, send = call(
        combine_kernel,
        [vec(3 * nb), vec(3 * nb)],
        [VM] * (STEPS + 2),
        [VM, VM],
        flops=6 * (STEPS + 1) * own.size,
        bytes_=(STEPS + 1 + 3) * own.size * 4,
        name="combine",
    )(*basis, weights)
    other = permute(send, swap)
    own_half = (lax.broadcasted_iota(jnp.int32, (1, width), 1) // half) == core[0]
    whole = jnp.where(own_half[None], mine, other).reshape(3, nb * rows, width)
    return start_point + whole[0], whole[1], whole[2]


def reduce_moments(local, devices):
    pairs = devices // 2
    if pairs & (pairs - 1):
        index = lax.axis_index("dom")
        slot = (lax.broadcasted_iota(jnp.int32, (2, 1, 1), 0) == index % 2).astype(F32)
        both = lax.psum(local[None] * slot, "dom")
        return jnp.where(index % 2 == 0, both[0], both[1])
    bit = 2
    while bit < devices:
        masks = [bit, 2 * bit, 3 * bit] if 2 * bit < devices else [bit]
        parts = [lax.ppermute(local, "dom", [(i, i ^ m) for i in range(devices)]) for m in masks]
        for part in parts:
            local = local + part
        bit *= 4
    return local


def solution(mesh):
    devices = mesh.shape["dom"]
    return jax.shard_map(
        functools.partial(shards, devices),
        mesh=mesh,
        in_specs=(
            P("dom", None),
            P("dom", None),
            P("dom", None),
            P("dom", None, None),
            P("dom", None),
            P("dom", None, None, None),
        ),
        out_specs=(P("dom", None), P("dom", None), P("dom", None)),
        check_vma=False,
    )
```

```python
import functools
import jax
import jax.numpy as jnp
from jax import lax
from jax.experimental import pallas as pl
from jax.experimental.pallas import tpu as pltpu
from jax.sharding import PartitionSpec as P

STEPS = 6
CENTER = 4.5
HALF = 4.5
F32 = jnp.float32
BF16 = jnp.bfloat16
VM = pl.BlockSpec(memory_space=pltpu.VMEM)
SM = pl.BlockSpec(memory_space=pltpu.SMEM)


def call(body, out_shape, in_specs, out_specs, scratch=(), flops=0, bytes_=0, name=None, grid=None):
    extra = {} if grid is None else {"grid": grid}
    return pl.pallas_call(
        body,
        out_shape=out_shape,
        in_specs=in_specs,
        out_specs=out_specs,
        scratch_shapes=list(scratch),
        cost_estimate=pl.CostEstimate(flops=flops, bytes_accessed=bytes_, transcendentals=0),
        name=name,
        compiler_params=pltpu.CompilerParams(vmem_limit_bytes=12 * 2**20),
        **extra,
    )


def pack_kernel(core, p_ref, r_ref, mine_ref, send_ref):
    half = p_ref.shape[1] // 2
    p, r = p_ref[...], r_ref[...]
    low = lax.broadcasted_iota(jnp.int32, p.shape, 1) < half
    first = jnp.where(low, p, pltpu.roll(r, half, 1))
    second = jnp.where(low, pltpu.roll(p, half, 1), r)
    is_first = core[0] == 0
    mine_ref[...] = jnp.where(is_first, first, second)
    send_ref[...] = jnp.where(is_first, second, first)


def copy_halo(core, lists, own, right_ref, left_ref):
    nb = right_ref.shape[0] - lists.shape[2]
    k = core[0]
    for target, whole, part, m in ((right_ref, 1, 0, 3), (left_ref, 0, 1, 1)):
        whole_slot = jnp.bitwise_xor(k, whole)
        part_slot = jnp.bitwise_xor(k, part)
        for b in range(nb):
            target[b] = own[whole_slot * nb + b]
        for e in range(lists.shape[2]):
            target[nb + e] = own[part_slot * nb + lists[part_slot, m, e]]


def first_kernel(core, lists, mine_ref, other_ref, own_ref, right_ref, left_ref):
    nb = mine_ref.shape[0]
    own_ref[:nb] = mine_ref[...]
    own_ref[nb:] = other_ref[...]
    copy_halo(core, lists, own_ref, right_ref, left_ref)


def index_kernel(core, lists, from_right, from_left, cols, out):
    k = core[0]
    cap = lists.shape[2]
    _, nb, slots = cols.shape
    right = 2 * nb
    left = 3 * nb + cap
    for s in range(2):
        t = jnp.bitwise_xor(k, s)
        is0 = t == 0
        other = 1 - s
        for b in range(nb):
            for j in range(slots):
                c = cols[s, b, j]
                place = s * nb + c
                for m in range(4):
                    for e in range(cap):
                        if m == 0:
                            v = jnp.where(is0, other * nb + lists[other, 0, e], right + from_right[k, 0, e])
                        elif m == 1:
                            v = jnp.where(is0, right + from_right[k, 1, e], right + nb + e)
                        elif m == 2:
                            v = jnp.where(is0, left + from_left[1 - k, 2, e], other * nb + lists[other, 2, e])
                        else:
                            v = jnp.where(is0, left + nb + e, left + from_left[1 - k, 3, e])
                        place = jnp.where(c == nb + m * cap + e, v, place)
                out[s * nb + b, j] = place


def matrix_kernel(a_ref, hi_ref, lo_ref):
    slots, rows, cols = a_ref.shape[1:]
    diag = lax.broadcasted_iota(jnp.int32, (rows, cols), 0) == lax.broadcasted_iota(
        jnp.int32, (rows, cols), 1
    )
    for j in range(slots):
        a = a_ref[0, j]
        if j == 0:
            a = a - jnp.where(diag, F32(CENTER), F32(0.0))
        a = a * F32(1.0 / HALF)
        hi = a.astype(BF16)
        hi_ref[0, :, j * cols : (j + 1) * cols] = hi
        lo_ref[0, :, j * cols : (j + 1) * cols] = (a - hi.astype(F32)).astype(BF16)


def step_kernel(last, core, lists, index, own_ref, fr_ref, fl_ref, h0, l0, h1, l1, new_ref, *rest):
    if last:
        (table,) = rest
    else:
        right_ref, left_ref, table = rest
    n_own, rows, width = own_ref.shape
    place = 0
    for ref in (own_ref, fr_ref, fl_ref):
        for b in range(ref.shape[0]):
            v = ref[b]
            hi = v.astype(BF16)
            table[place, :, :width] = hi
            table[place, :, width:] = (v - hi.astype(F32)).astype(BF16)
            place += 1
    half = n_own // 2
    slots = index.shape[1]
    for i in range(n_own):
        h, l = (h0, l0) if i < half else (h1, l1)
        acc = None
        for j in range(0, slots, 2):
            cols = [table[index[i, q]] for q in range(j, min(j + 2, slots))]
            tile = jnp.concatenate(cols, axis=0) if len(cols) > 1 else cols[0]
            span = slice(j * rows, (j + len(cols)) * rows)
            for part in (h, l):
                d = jnp.dot(part[i % half, :, span], tile, preferred_element_type=F32)
                acc = d if acc is None else acc + d
        new_ref[i] = acc[:, :width] + acc[:, width:]
    if not last:
        copy_halo(core, lists, new_ref, right_ref, left_ref)


def fold(x):
    return jnp.sum(x.reshape(-1, 8, x.shape[-1]), axis=0)


def moment_kernel(first, *refs):
    if first:
        now_ref, out = refs
        prev_ref = None
    else:
        now_ref, prev_ref, out = refs
    blocks, rows, width = now_ref.shape
    half = width // 2
    acc = [jnp.zeros((8, width), F32) for _ in range(4)]
    for b in range(blocks):
        s = now_ref[b]
        turned = pltpu.roll(s, half, 1)
        acc[1] += fold(s * s)
        acc[3] += fold(s * turned)
        if prev_ref is not None:
            q = prev_ref[b]
            acc[0] += fold(s * q)
            acc[2] += fold(s * pltpu.roll(q, half, 1))
    for i in range(4):
        out[i : i + 1, :] = jnp.sum(acc[i], axis=0, keepdims=True)
    out[4:8, :] = jnp.zeros((4, width), F32)


def coefficient_kernel(m_ref, out_ref, gram_ref):
    width = m_ref.shape[1]
    half = width // 2
    count = STEPS + 1

    def row(j, i):
        return m_ref[8 * j + i : 8 * j + i + 1, :]

    def moment(n):
        j = (n + 1) // 2
        return row(j, 0 if n % 2 else 1)

    def cross(n):
        j = (n + 1) // 2
        return row(j, 2 if n % 2 else 3)

    size = gram_ref.shape[1]
    gram_ref[...] = jnp.zeros(gram_ref.shape, F32)
    for a in range(count):
        for b in range(count):
            gram_ref[a, b : b + 1, :] = moment(a + b)
            if b < STEPS:
                gram_ref[a, count + b : count + b + 1, :] = cross(a + b)
            if a < STEPS:
                gram_ref[count + a, b : b + 1, :] = cross(a + b)
            if a < STEPS and b < STEPS:
                gram_ref[count + a, count + b : count + b + 1, :] = pltpu.roll(moment(a + b), half, 1)
    ids = lax.broadcasted_iota(jnp.int32, (size, width), 0)
    active = (ids < STEPS) | ((ids > STEPS) & (ids < 2 * STEPS))

    def change(v):
        v = jnp.where(active, v, F32(0.0))
        return F32(CENTER) * v + F32(HALF) * pltpu.roll(v, 1, 0)

    def times(v):
        out = None
        for a in range(2 * STEPS + 1):
            t = gram_ref[a] * v[a : a + 1, :]
            out = t if out is None else out + t
        return out

    def dot(u, v):
        return jnp.sum(u * v, axis=0, keepdims=True)

    x = jnp.zeros((size, width), F32)
    r = jnp.where(ids == STEPS + 1, F32(1.0), F32(0.0))
    d = jnp.where(ids == 0, F32(1.0), F32(0.0))
    current = dot(r, times(r))
    for _ in range(STEPS):
        moved = change(d)
        alpha = current / dot(d, times(moved))
        x = x + alpha * d
        r = r - alpha * moved
        following = dot(r, times(r))
        d = r + (following / current) * d
        current = following
    low = lax.broadcasted_iota(jnp.int32, (8, width), 1) < half
    sub = lax.broadcasted_iota(jnp.int32, (8, width), 0)
    for q, v in enumerate((x, r, d)):
        lows = v[:8]
        lows = jnp.where(sub < count, lows, F32(0.0))
        highs = pltpu.roll(v, size - count, 0)[:8]
        highs = jnp.where(sub < STEPS, pltpu.roll(highs, half, 1), F32(0.0))
        out_ref[8 * q : 8 * q + 8, :] = jnp.where(low, lows, highs)


def combine_kernel(*refs):
    basis, (w_ref, mine_ref, send_ref) = refs[:-3], refs[-3:]
    blocks, rows, width = basis[0].shape
    half = width // 2
    nb = blocks // 2
    for b in range(blocks):
        vs = [s[b] for s in basis]
        for q in range(3):
            out = None
            for j, v in enumerate(vs):
                t = v * w_ref[8 * q + j : 8 * q + j + 1, :]
                out = t if out is None else out + t
            out = out + pltpu.roll(out, half, 1)
            if b < nb:
                mine_ref[q * nb + b] = out
            else:
                send_ref[q * nb + b - nb] = out


def shards(devices, start_point, residual, direction, send_list, block_cols, block_vals):
    nb, slots, rows, _ = block_vals.shape
    cap = send_list.shape[2]
    width = direction.shape[1]
    half = width // 2
    ghosts = nb + cap
    sds = jax.ShapeDtypeStruct
    vec = lambda n: sds((n, rows, width), F32)
    core = (lax.axis_index("dom") % 2).astype(jnp.int32).reshape(1)
    swap = [(i, i ^ 1) for i in range(devices)]
    to_right = [(i, (i + 2) % devices) for i in range(devices)]
    to_left = [(i, (i - 2) % devices) for i in range(devices)]
    permute = lambda v, pairs: lax.ppermute(v, "dom", pairs)

    mine, send = call(
        pack_kernel,
        [sds(direction.shape, F32)] * 2,
        [SM, VM, VM],
        [VM, VM],
        bytes_=4 * direction.size * 4,
        flops=direction.size,
        name="pack",
    )(core, direction, residual)
    other = permute(send, swap)
    lists = jnp.stack([send_list[0], permute(send_list[0], swap)])
    own, right, left = call(
        first_kernel,
        [vec(2 * nb), vec(ghosts), vec(ghosts)],
        [SM, SM, VM, VM],
        [VM, VM, VM],
        bytes_=6 * direction.size * 4,
        flops=direction.size,
        name="first",
    )(core, lists, mine.reshape(nb, rows, width), other.reshape(nb, rows, width))
    fr, fl = permute(left, to_left), permute(right, to_right)
    vals_other = permute(block_vals, swap)
    cols = jnp.stack([block_cols, permute(block_cols, swap)])
    lists_right, lists_left = permute(lists, to_left), permute(lists, to_right)
    index = call(
        index_kernel,
        sds((2 * nb, slots), jnp.int32),
        [SM] * 5,
        SM,
        flops=1000,
        name="index",
    )(core, lists, lists_right, lists_left, cols)

    def split(vals):
        spec = pl.BlockSpec((1, rows, slots * rows), lambda i: (i, 0, 0))
        return call(
            matrix_kernel,
            [sds((nb, rows, slots * rows), BF16)] * 2,
            [pl.BlockSpec((1, slots, rows, rows), lambda i: (i, 0, 0, 0))],
            [spec, spec],
            grid=(nb,),
            flops=4 * vals.size,
            bytes_=8 * vals.size,
            name="matrix",
        )(vals)

    parts = split(block_vals) + split(vals_other)
    basis = [own]
    moments = []

    def moment(j):
        args = basis[j : j + 1] + basis[j - 1 : j] if j else basis[:1]
        moments.append(
            call(
                functools.partial(moment_kernel, j == 0),
                sds((8, width), F32),
                [VM] * len(args),
                VM,
                flops=8 * own.size,
                bytes_=8 * own.size,
                name="moment",
            )(*args)
        )

    for j in range(STEPS):
        last = j == STEPS - 1
        out = [vec(2 * nb)] + ([] if last else [vec(ghosts), vec(ghosts)])
        res = call(
            functools.partial(step_kernel, last),
            out,
            [SM] * 3 + [VM] * 7,
            [VM] * len(out),
            scratch=[pltpu.VMEM((2 * nb + 2 * ghosts, rows, 2 * width), BF16)],
            flops=2 * 4 * 2 * nb * slots * rows * rows * width,
            bytes_=8 * 2 * nb * slots * rows * rows,
            name="step",
        )(core, lists, index, basis[-1], fr, fl, *parts)
        moment(j)
        basis.append(res[0])
        if not last:
            fr, fl = permute(res[2], to_left), permute(res[1], to_right)
    moment(STEPS)
    total = reduce_moments(jnp.concatenate(moments, axis=0), devices)
    weights = call(
        coefficient_kernel,
        sds((24, width), F32),
        [VM],
        VM,
        scratch=[pltpu.VMEM((2 * STEPS + 1, 16, width), F32)],
        flops=100000,
        name="coefficients",
    )(total)
    mine, send = call(
        combine_kernel,
        [vec(3 * nb), vec(3 * nb)],
        [VM] * (STEPS + 2),
        [VM, VM],
        flops=6 * (STEPS + 1) * own.size,
        bytes_=(STEPS + 1 + 3) * own.size * 4,
        name="combine",
    )(*basis, weights)
    other = permute(send, swap)
    own_half = (lax.broadcasted_iota(jnp.int32, (1, width), 1) // half) == core[0]
    whole = jnp.where(own_half[None], mine, other).reshape(3, nb * rows, width)
    return start_point + whole[0], whole[1], whole[2]


def reduce_moments(local, devices):
    pairs = devices // 2
    if pairs & (pairs - 1):
        index = lax.axis_index("dom")
        slot = (lax.broadcasted_iota(jnp.int32, (2, 1, 1), 0) == index % 2).astype(F32)
        both = lax.psum(local[None] * slot, "dom")
        return jnp.where(index % 2 == 0, both[0], both[1])
    bit = 2
    while bit < devices:
        masks = [bit, 2 * bit, 3 * bit] if 2 * bit < devices else [bit]
        parts = [lax.ppermute(local, "dom", [(i, i ^ m) for i in range(devices)]) for m in masks]
        for part in parts:
            local = local + part
        bit *= 4
    return local


def solution(mesh):
    devices = mesh.shape["dom"]
    return jax.shard_map(
        functools.partial(shards, devices),
        mesh=mesh,
        in_specs=(
            P("dom", None),
            P("dom", None),
            P("dom", None),
            P("dom", None, None),
            P("dom", None),
            P("dom", None, None, None),
        ),
        out_specs=(P("dom", None), P("dom", None), P("dom", None)),
        check_vma=False,
    )
```

```python
import functools
import jax
import jax.numpy as jnp
from jax import lax
from jax.experimental import pallas as pl
from jax.experimental.pallas import tpu as pltpu
from jax.sharding import PartitionSpec as P

STEPS = 6
CENTER = 4.5
HALF = 4.5
F32 = jnp.float32
BF16 = jnp.bfloat16
VM = pl.BlockSpec(memory_space=pltpu.VMEM)
SM = pl.BlockSpec(memory_space=pltpu.SMEM)


def call(body, out_shape, in_specs, out_specs, scratch=(), flops=0, bytes_=0, name=None, grid=None):
    extra = {} if grid is None else {"grid": grid}
    return pl.pallas_call(
        body,
        out_shape=out_shape,
        in_specs=in_specs,
        out_specs=out_specs,
        scratch_shapes=list(scratch),
        cost_estimate=pl.CostEstimate(flops=flops, bytes_accessed=bytes_, transcendentals=0),
        name=name,
        compiler_params=pltpu.CompilerParams(vmem_limit_bytes=12 * 2**20),
        **extra,
    )


def halves(shape):
    return lax.broadcasted_iota(jnp.int32, shape, len(shape) - 1) < shape[-1] // 2


def pack_kernel(core, v_ref, mine_ref, send_ref):
    rows, width = v_ref.shape[1:]
    top, bottom = v_ref[:, : rows // 2], v_ref[:, rows // 2 :]
    low = halves(top.shape)
    first = jnp.where(low, top, pltpu.roll(bottom, width // 2, 2))
    second = jnp.where(low, pltpu.roll(top, width // 2, 2), bottom)
    is_first = core[0] == 0
    mine_ref[...] = jnp.where(is_first, first, second)
    send_ref[...] = jnp.where(is_first, second, first)


def copy_halo(core, lists, own, right_ref, left_ref):
    nb = right_ref.shape[0] - lists.shape[2]
    k = core[0]
    for target, whole, part, m in ((right_ref, 1, 0, 3), (left_ref, 0, 1, 1)):
        whole_slot = jnp.bitwise_xor(k, whole)
        part_slot = jnp.bitwise_xor(k, part)
        for b in range(nb):
            target[b] = own[whole_slot * nb + b]
        for e in range(lists.shape[2]):
            target[nb + e] = own[part_slot * nb + lists[part_slot, m, e]]


def first_kernel(core, lists, mine_ref, other_ref, own_ref, right_ref, left_ref):
    nb = mine_ref.shape[0]
    own_ref[:nb] = mine_ref[...]
    own_ref[nb:] = other_ref[...]
    copy_halo(core, lists, own_ref, right_ref, left_ref)


def index_kernel(core, lists, from_right, from_left, cols, out, place):
    k = core[0]
    cap = lists.shape[2]
    _, nb, slots = cols.shape
    right = 2 * nb
    left = 3 * nb + cap
    for s in range(2):
        is0 = jnp.bitwise_xor(k, s) == 0
        other = 1 - s
        for b in range(nb):
            place[b] = s * nb + b
        for e in range(cap):
            place[nb + e] = jnp.where(is0, other * nb + lists[other, 0, e], right + from_right[k, 0, e])
            place[nb + cap + e] = jnp.where(is0, right + from_right[k, 1, e], right + nb + e)
            place[nb + 2 * cap + e] = jnp.where(
                is0, left + from_left[1 - k, 2, e], other * nb + lists[other, 2, e]
            )
            place[nb + 3 * cap + e] = jnp.where(is0, left + nb + e, left + from_left[1 - k, 3, e])
        for b in range(nb):
            for j in range(slots):
                out[s * nb + b, j] = place[cols[s, b, j]]


def matrix_kernel(a_ref, hi_ref, lo_ref):
    slots, rows, cols = a_ref.shape[1:]
    diag = lax.broadcasted_iota(jnp.int32, (rows, cols), 0) == lax.broadcasted_iota(
        jnp.int32, (rows, cols), 1
    )
    for j in range(slots):
        a = a_ref[0, j]
        if j == 0:
            a = a - jnp.where(diag, F32(CENTER), F32(0.0))
        a = a * F32(1.0 / HALF)
        hi = a.astype(BF16)
        hi_ref[0, :, j * cols : (j + 1) * cols] = hi
        lo_ref[0, :, j * cols : (j + 1) * cols] = (a - hi.astype(F32)).astype(BF16)


def step_kernel(last, core, lists, index, own_ref, fr_ref, fl_ref, h0, l0, h1, l1, new_ref, *rest):
    if last:
        (table,) = rest
    else:
        right_ref, left_ref, table = rest
    n_own, cut, width = own_ref.shape
    rows, half = 2 * cut, width // 2
    low = halves((cut, width))
    place = 0
    for ref in (own_ref, fr_ref, fl_ref):
        for b in range(ref.shape[0]):
            v = ref[b]
            hi = v.astype(BF16).astype(F32)
            lo = v - hi
            table[place, :cut] = jnp.where(low, hi, pltpu.roll(lo, half, 1)).astype(BF16)
            table[place, cut:] = jnp.where(low, pltpu.roll(hi, half, 1), lo).astype(BF16)
            place += 1
    slots = index.shape[1]
    for i in range(n_own):
        h, l = (h0, l0) if i < n_own // 2 else (h1, l1)
        acc = None
        for j in range(0, slots, 2):
            cols = [table[index[i, q]] for q in range(j, min(j + 2, slots))]
            tile = jnp.concatenate(cols, axis=0) if len(cols) > 1 else cols[0]
            span = slice(j * rows, (j + len(cols)) * rows)
            for part in (h, l):
                d = jnp.dot(part[i % (n_own // 2), :, span], tile, preferred_element_type=F32)
                acc = d if acc is None else acc + d
        acc = acc + pltpu.roll(acc, half, 1)
        new_ref[i] = jnp.where(low, acc[:cut], acc[cut:])
    if not last:
        copy_halo(core, lists, new_ref, right_ref, left_ref)


def fold(x):
    return jnp.sum(x.reshape(-1, 8, x.shape[-1]), axis=0)


def moment_kernel(pairs, *refs):
    out = refs[-1]
    blocks, _, width = refs[0].shape
    acc = [None] * 8
    for b in range(blocks):
        v = [ref[b] for ref in refs[:-1]]
        for i, pair in enumerate(pairs):
            if pair is not None:
                t = fold(v[pair[0]] * v[pair[1]])
                acc[i] = t if acc[i] is None else acc[i] + t
    for i in range(8):
        if acc[i] is None:
            out[i : i + 1, :] = jnp.zeros((1, width), F32)
        else:
            out[i : i + 1, :] = jnp.sum(acc[i], axis=0, keepdims=True)


def coefficient_kernel(m_ref, out_ref, gram_ref, sum_ref):
    width = m_ref.shape[1]
    count = STEPS + 1
    sum_ref[...] = m_ref[...] + pltpu.roll(m_ref[...], width // 2, 1)

    def moment(kind, n):
        at = 8 * ((n + 1) // 2) + 2 * kind + (0 if n % 2 else 1)
        return sum_ref[at : at + 1, :]

    size = gram_ref.shape[1]
    gram_ref[...] = jnp.zeros(gram_ref.shape, F32)
    for a in range(count):
        for b in range(count):
            gram_ref[a, b : b + 1, :] = moment(0, a + b)
            if b < STEPS:
                gram_ref[a, count + b : count + b + 1, :] = moment(1, a + b)
            if a < STEPS:
                gram_ref[count + a, b : b + 1, :] = moment(1, a + b)
            if a < STEPS and b < STEPS:
                gram_ref[count + a, count + b : count + b + 1, :] = moment(2, a + b)
    ids = lax.broadcasted_iota(jnp.int32, (size, width), 0)
    active = (ids < STEPS) | ((ids > STEPS) & (ids < 2 * STEPS))

    def change(v):
        v = jnp.where(active, v, F32(0.0))
        return F32(CENTER) * v + F32(HALF) * pltpu.roll(v, 1, 0)

    def times(v):
        out = None
        for a in range(2 * STEPS + 1):
            t = gram_ref[a] * v[a : a + 1, :]
            out = t if out is None else out + t
        return out

    def dot(u, v):
        return jnp.sum(u * v, axis=0, keepdims=True)

    x = jnp.zeros((size, width), F32)
    r = jnp.where(ids == STEPS + 1, F32(1.0), F32(0.0))
    d = jnp.where(ids == 0, F32(1.0), F32(0.0))
    current = dot(r, times(r))
    for _ in range(STEPS):
        moved = change(d)
        alpha = current / dot(d, times(moved))
        x = x + alpha * d
        r = r - alpha * moved
        following = dot(r, times(r))
        d = r + (following / current) * d
        current = following
    for q, v in enumerate((x, r, d)):
        out_ref[size * q : size * (q + 1), :] = v


def combine_kernel(second, *refs):
    basis, (w_ref, out_ref) = refs[:-2], refs[-2:]
    nb = basis[0].shape[0] // 2
    size = w_ref.shape[0] // 3
    for b in range(nb):
        vs = [s[second * nb + b] for s in basis]
        for q in range(3):
            out = None
            for j, v in enumerate(vs):
                t = v * w_ref[size * q + j : size * q + j + 1, :]
                out = t if out is None else out + t
            out_ref[q * nb + b] = out


def unpack_kernel(core, start_ref, mine_ref, other_ref, *out_refs):
    nb, rows, width = start_ref.shape
    cut, half = rows // 2, width // 2
    is_first = core[0] == 0
    low = halves((cut, width))
    for q, out_ref in enumerate(out_refs):
        for b in range(nb):
            mine, other = mine_ref[q * nb + b], other_ref[q * nb + b]
            first = jnp.where(is_first, mine, other)
            second = jnp.where(is_first, other, mine)
            top = jnp.where(low, first, pltpu.roll(second, half, 1))
            bottom = jnp.where(low, pltpu.roll(first, half, 1), second)
            if q == 0:
                top = top + start_ref[b, :cut]
                bottom = bottom + start_ref[b, cut:]
            out_ref[b, :cut] = top
            out_ref[b, cut:] = bottom


def shards(devices, start_point, residual, direction, send_list, block_cols, block_vals):
    nb, slots, rows, _ = block_vals.shape
    cap = send_list.shape[2]
    width = direction.shape[1]
    cut = rows // 2
    ghosts = nb + cap
    sds = jax.ShapeDtypeStruct
    vec = lambda n: sds((n, cut, width), F32)
    core = (lax.axis_index("dom") % 2).astype(jnp.int32).reshape(1)
    swap = [(i, i ^ 1) for i in range(devices)]
    to_right = [(i, (i + 2) % devices) for i in range(devices)]
    to_left = [(i, (i - 2) % devices) for i in range(devices)]
    permute = lambda v, pairs: lax.ppermute(v, "dom", pairs)
    blocked = lambda v: v.reshape(nb, rows, width)
    size = direction.size

    lists = jnp.stack([send_list[0], permute(send_list[0], swap)])
    lists_right, lists_left = permute(lists, to_left), permute(lists, to_right)

    def pack(v):
        return call(
            pack_kernel, [vec(nb)] * 2, [SM, VM], [VM, VM], flops=4 * size, bytes_=8 * size, name="pack"
        )(core, blocked(v))

    def begin(mine, other):
        return call(
            first_kernel,
            [vec(2 * nb), vec(ghosts), vec(ghosts)],
            [SM, SM, VM, VM],
            [VM, VM, VM],
            flops=4 * size,
            bytes_=12 * size,
            name="first",
        )(core, lists, mine, other)

    def exchange(right, left):
        return permute(left, to_left), permute(right, to_right)

    packed = [pack(v) for v in (direction, residual)]
    started = [begin(mine, permute(send, swap)) for mine, send in packed]
    halo = [exchange(right, left) for _, right, left in started]
    p_basis, r_basis = ([own] for own, _, _ in started)

    vals_other = permute(block_vals, swap)
    cols = jnp.stack([block_cols, permute(block_cols, swap)])
    index = call(
        index_kernel,
        sds((2 * nb, slots), jnp.int32),
        [SM] * 5,
        SM,
        scratch=[pltpu.SMEM((nb + 4 * cap,), jnp.int32)],
        flops=1000,
        name="index",
    )(core, lists, lists_right, lists_left, cols)

    def split(vals):
        spec = pl.BlockSpec((1, rows, slots * rows), lambda i: (i, 0, 0))
        return call(
            matrix_kernel,
            [sds((nb, rows, slots * rows), BF16)] * 2,
            [pl.BlockSpec((1, slots, rows, rows), lambda i: (i, 0, 0, 0))],
            [spec, spec],
            grid=(nb,),
            flops=4 * vals.size,
            bytes_=8 * vals.size,
            name="matrix",
        )(vals)

    parts = split(block_vals) + split(vals_other)
    moments = []

    def moment(j):
        now_r = j < STEPS
        args = [p_basis[j]] + ([r_basis[j]] if now_r else [])
        if j:
            args += [p_basis[j - 1], r_basis[j - 1]]
        p, r = 0, 1
        q, s = len(args) - 2, len(args) - 1
        pairs = [
            (p, q) if j else None,
            (p, p),
            (p, s) if j else None,
            (p, r) if now_r else None,
            (r, s) if j and now_r else None,
            (r, r) if now_r else None,
        ]
        moments.append(
            call(
                functools.partial(moment_kernel, pairs),
                sds((8, width), F32),
                [VM] * len(args),
                VM,
                flops=12 * size,
                bytes_=16 * size,
                name="moment",
            )(*args)
        )

    def step(v, halo, last):
        out = [vec(2 * nb)] + ([] if last else [vec(ghosts), vec(ghosts)])
        return call(
            functools.partial(step_kernel, last),
            out,
            [SM] * 3 + [VM] * 7,
            [VM] * len(out),
            scratch=[pltpu.VMEM((2 * nb + 2 * ghosts, rows, width), BF16)],
            flops=2 * 4 * 2 * nb * slots * rows * rows * width,
            bytes_=8 * 2 * nb * slots * rows * rows,
            name="step",
        )(core, lists, index, v, *halo, *parts)

    for j in range(STEPS):
        for which, (basis, count) in enumerate(((p_basis, STEPS), (r_basis, STEPS - 1))):
            if j < count:
                last = j == count - 1
                res = step(basis[-1], halo[which], last)
                basis.append(res[0])
                if not last:
                    halo[which] = exchange(res[1], res[2])
        moment(j)
    moment(STEPS)
    total = reduce_moments(jnp.concatenate(moments, axis=0), devices)
    lanes = 16
    weights = call(
        coefficient_kernel,
        sds((3 * lanes, width), F32),
        [VM],
        VM,
        scratch=[
            pltpu.VMEM((2 * STEPS + 1, lanes, width), F32),
            pltpu.VMEM(total.shape, F32),
        ],
        flops=100000,
        name="coefficients",
    )(total)
    basis = p_basis + r_basis

    def combine(second):
        return call(
            functools.partial(combine_kernel, second),
            vec(3 * nb),
            [VM] * (len(basis) + 1),
            VM,
            flops=6 * len(basis) * size // 2,
            bytes_=4 * (len(basis) + 3) * size // 2,
            name="combine",
        )(*basis, weights)

    other = permute(combine(1), swap)
    outs = call(
        unpack_kernel,
        [sds((nb, rows, width), F32)] * 3,
        [SM, VM, VM, VM],
        [VM] * 3,
        flops=6 * size,
        bytes_=28 * size,
        name="unpack",
    )(core, blocked(start_point), combine(0), other)
    return tuple(o.reshape(start_point.shape) for o in outs)


def reduce_moments(local, devices):
    pairs = devices // 2
    if pairs & (pairs - 1):
        index = lax.axis_index("dom")
        slot = (lax.broadcasted_iota(jnp.int32, (2, 1, 1), 0) == index % 2).astype(F32)
        both = lax.psum(local[None] * slot, "dom")
        return jnp.where(index % 2 == 0, both[0], both[1])
    bit = 2
    while bit < devices:
        masks = [bit, 2 * bit, 3 * bit] if 2 * bit < devices else [bit]
        parts = [lax.ppermute(local, "dom", [(i, i ^ m) for i in range(devices)]) for m in masks]
        for part in parts:
            local = local + part
        bit *= 4
    return local


def solution(mesh):
    devices = mesh.shape["dom"]
    return jax.shard_map(
        functools.partial(shards, devices),
        mesh=mesh,
        in_specs=(
            P("dom", None),
            P("dom", None),
            P("dom", None),
            P("dom", None, None),
            P("dom", None),
            P("dom", None, None, None),
        ),
        out_specs=(P("dom", None), P("dom", None), P("dom", None)),
        check_vma=False,
    )
```
